128 devices in a mesh: blk: 32 (over x, z, core), grp: 4 (over y).
Axes of the slice: x: 4, y: 4, z: 4, core: 2. Of those that a mesh axis runs over, the one named last changes fastest.
Arguments:
- statistics: float32 [4, 64, 512, 512], P('grp', 'blk'), as said below
- gradients: bfloat16 [4, 16, 512, 14336], P('grp', None, None, 'blk'), may hold values from -6 to 6
- live_counts: int32 [4, 32], P('grp'), may hold values from 0 to 2, as said below
- slot_row: int32 [4, 64], P('grp'), may hold values from 0 to 15, as said below
- sweeps: int32 [4, 64], P('grp', 'blk'), may hold values from 1 to 2, as said below
Outputs:
- updates: bfloat16 [4, 16, 512, 14336], P('grp', None, None, 'blk')
- off_max: float32 [2], replicated
The draws below stay inside these ranges and needn't reach their ends.
Inputs may be any that keep to these rules, and one draw needn't show every extreme that they name: `live_counts`: the live slots of one index of grp number exactly 16; in every draw some device of each grp index has 2 live slots. `slot_row`: over the live slots of one index of grp each row block 0 to 15 appears exactly once. In each index of grp some live slot has 2 sweeps. `statistics`: every block is symmetric positive definite.
All inputs are finite; a program needn't handle non-finite values.
Results may differ from the reference program's by a relative error of at most 0.0051.
Values may be sent and summed in bfloat16 or wider, within the bound.
No kernel may reach another device: no remote copies, remote signals or barrier semaphores. Data moves between devices by JAX's collectives and lax.ppermute only.
A program may use at most 192 MiB of HBM per device.

```python
import jax
import jax.numpy as jnp
from jax import lax

FF = 14336
BLOCK = 512
SLOTS = 2
ROWB = 16
MAXS = 2
N_BLK = 32
N_GRP = 4


def layout(base_key):
    slot_total = N_BLK * SLOTS

    def one_group(row_key):
        keys_list = jax.random.split(row_key, 5)
        heavy_owner = jax.random.randint(keys_list[0], (), 0, N_BLK)
        partner_owner = (heavy_owner + N_BLK // 2) % N_BLK
        priority = jax.random.permutation(keys_list[1], slot_total).astype(jnp.int32)
        slot_ids = lax.iota(jnp.int32, slot_total)
        owner_of = slot_ids // SLOTS
        local_slot = slot_ids % SLOTS
        priority = jnp.where(owner_of == heavy_owner, local_slot - SLOTS, priority)
        priority = jnp.where(owner_of == partner_owner, slot_total + local_slot, priority)
        ranking = jnp.argsort(priority, stable=True)
        picked = jnp.zeros((slot_total,), jnp.int32).at[ranking[:ROWB]].set(1)
        counts = jnp.sum(picked.reshape(N_BLK, SLOTS), axis=1).astype(jnp.int32)
        offsets = jnp.cumsum(counts) - counts
        live_slot = local_slot < counts[owner_of]
        row_order = jax.random.permutation(keys_list[2], ROWB).astype(jnp.int32)
        position = jnp.clip(offsets[owner_of] + local_slot, 0, ROWB - 1)
        filler = jax.random.randint(keys_list[3], (slot_total,), 0, ROWB)
        rows_drawn = jnp.where(live_slot, row_order[position], filler).astype(jnp.int32)
        sweep_drawn = jax.random.randint(keys_list[4], (slot_total,), 1, MAXS + 1)
        sweep_drawn = jnp.where(slot_ids == heavy_owner * SLOTS, MAXS, sweep_drawn).astype(jnp.int32)
        return (counts, rows_drawn, sweep_drawn)
    return jax.vmap(one_group)(jax.random.split(jax.random.fold_in(base_key, 11), N_GRP))


def draw_live_counts(key, part):
    return layout(key)[0]


def draw_slot_row(key, part):
    return layout(key)[1]


def draw_sweeps(key, part):
    return layout(key)[2]


def draw_statistics(key, part):
    slot_total = N_BLK * SLOTS
    samples = 2 * BLOCK
    item_keys = jax.random.split(jax.random.fold_in(key, 5), N_GRP * slot_total)

    def one_block(item_key):
        keys_list = jax.random.split(item_key, 2)
        noise = jax.random.normal(keys_list[0], (BLOCK, samples), jnp.float32)
        scales = jnp.exp(jax.random.uniform(keys_list[1], (BLOCK,), jnp.float32, 0.0, jnp.log(10.0)))
        product = jnp.dot(noise, noise.T, precision=lax.Precision.HIGHEST) / samples
        product = 0.5 * (product + product.T)
        return scales[:, None] * product * scales[None, :] + 0.05 * jnp.eye(BLOCK, dtype=jnp.float32)
    blocks_all = lax.map(one_block, item_keys)
    return blocks_all.reshape(N_GRP, slot_total, BLOCK, BLOCK)


def shard_levels(own_key, shape, shards, least, high):
    gain = 1.0
    for axis_at, shards_of in shards:
        steps = jax.random.uniform(jax.random.fold_in(jax.random.fold_in(own_key, 6), axis_at), (shards_of,), jnp.float32, least / len(shards), high / len(shards))
        gain = gain * jnp.repeat(jnp.exp(steps), shape[axis_at] // shards_of).reshape((-1,) + (1,) * (len(shape) - 1 - axis_at))
    return gain


def scatter_about(key, shape, spread, bound, cuts=(), kind=jnp.bfloat16):
    factor_of = shard_levels(key, shape, cuts, -0.22, 0.18) if cuts else 1.0
    drawn = jax.random.normal(key, shape, jnp.float32) * spread * factor_of
    return jnp.minimum(jnp.maximum(drawn, -bound), bound).astype(kind)


def setup_inputs(seed: int = 0) -> dict:
    arg_keys = jax.random.split(jax.random.key(seed), 6)
    statistics = draw_statistics(jax.random.fold_in(arg_keys[5], 71), 0)
    gradients = scatter_about(arg_keys[1], (N_GRP, ROWB, BLOCK, FF), 1.0, 6.0, ((0, 4), (3, 32)))
    live_counts = draw_live_counts(jax.random.fold_in(arg_keys[5], 71), 0)
    slot_row = draw_slot_row(jax.random.fold_in(arg_keys[5], 71), 0)
    sweeps = draw_sweeps(jax.random.fold_in(arg_keys[5], 71), 0)
    return dict(statistics=statistics, gradients=gradients, live_counts=live_counts, slot_row=slot_row, sweeps=sweeps)


damping = 0.01
pairings = ((0, 1, 2, 3), (0, 2, 1, 3), (0, 3, 1, 2))
highest = lax.Precision.HIGHEST

def regroup_cols(values, pairing, group_width):
    return jnp.concatenate([values[:, member * group_width:(member + 1) * group_width] for member in pairing], axis=1)

def regroup(values, pairing, group_width):
    stacked = jnp.concatenate([values[member * group_width:(member + 1) * group_width] for member in pairing], axis=0)
    return regroup_cols(stacked, pairing, group_width)

def generator(square_sub):
    group_width = square_sub.shape[-1] // 2
    diagonal = jnp.diagonal(square_sub, axis1=1, axis2=2)
    lower_diag = diagonal[:, :group_width, None]
    upper_diag = diagonal[:, None, group_width:]
    coupling = square_sub[:, :group_width, group_width:]
    difference = upper_diag - lower_diag
    bottom = difference * difference + 4.0 * coupling * coupling + damping * (lower_diag + upper_diag) ** 2
    angles = coupling * difference / bottom
    blank = jnp.zeros_like(angles)
    top_half = jnp.concatenate([blank, angles], axis=2)
    low_half = jnp.concatenate([-jnp.swapaxes(angles, 1, 2), blank], axis=2)
    return jnp.concatenate([top_half, low_half], axis=1)

def cayley(skew_part):
    order_size = skew_part.shape[-1]
    identity = jnp.eye(order_size, dtype=jnp.float32)
    square = jnp.einsum('hij,hjk->hik', skew_part, skew_part, precision=highest)
    numerator = identity + skew_part + 0.25 * square
    denominator = identity - 0.25 * square
    factor = jnp.linalg.cholesky(denominator)
    return jax.scipy.linalg.cho_solve((factor, True), numerator)

def rotate_round(matrix, vectors, pairing):
    block_size = matrix.shape[0]
    group_width = block_size // 4
    restore = [pairing.index(member) for member in range(4)]
    matrix = regroup(matrix, pairing, group_width)
    vectors = regroup_cols(vectors, pairing, group_width)
    half_size = 2 * group_width
    square_sub = jnp.stack([matrix[:half_size, :half_size], matrix[half_size:, half_size:]])
    rotation = cayley(generator(square_sub))
    row_part = jnp.einsum('hpq,hpc->hqc', rotation, matrix.reshape(2, half_size, block_size), precision=highest)
    row_part = row_part.reshape(block_size, block_size)
    matrix = jnp.einsum('rhp,hpq->rhq', row_part.reshape(block_size, 2, half_size), rotation, precision=highest)
    matrix = matrix.reshape(block_size, block_size)
    vectors = jnp.einsum('rhp,hpq->rhq', vectors.reshape(block_size, 2, half_size), rotation, precision=highest)
    vectors = vectors.reshape(block_size, block_size)
    return (regroup(matrix, restore, group_width), regroup_cols(vectors, restore, group_width))

def one_sweep(matrix, vectors):
    for pairing in pairings:
        matrix, vectors = rotate_round(matrix, vectors, pairing)
    return (matrix, vectors)

def off_norm(matrix):
    block_size = matrix.shape[0]
    on_diagonal = lax.broadcasted_iota(jnp.int32, (block_size, block_size), 0) == lax.broadcasted_iota(jnp.int32, (block_size, block_size), 1)
    outside = jnp.where(on_diagonal, 0.0, matrix)
    return jnp.sqrt(jnp.sum(outside * outside) / jnp.sum(matrix * matrix))

def root_factor(matrix, vectors):
    scales = jnp.power(jnp.diagonal(matrix), -0.25)
    return jnp.dot(vectors * scales[None, :], vectors.T, precision=highest).astype(jnp.bfloat16)

def pick(group_stats, group_slots):
    return jnp.take(group_stats, group_slots, axis=0)

def reference(statistics, gradients, live_counts, slot_row, sweeps):
    slot_total = N_BLK * SLOTS
    slot_ids = lax.iota(jnp.int32, slot_total)
    row_ids = lax.iota(jnp.int32, ROWB)
    is_live = slot_ids[None, :] % SLOTS < jnp.repeat(live_counts, SLOTS, axis=1)
    matches = (slot_row[:, None, :] == row_ids[None, :, None]) & is_live[:, None, :]
    slot_of = lax.optimization_barrier(jnp.sum(jnp.where(matches, slot_ids[None, None, :], 0), axis=2)).astype(jnp.int32)
    chosen = jax.vmap(pick)(statistics, slot_of)
    chosen_sweeps = jax.vmap(pick)(sweeps, slot_of)
    blocks_flat = chosen.reshape(N_GRP * ROWB, BLOCK, BLOCK)
    sweeps_flat = chosen_sweeps.reshape(N_GRP * ROWB)
    identity = jnp.eye(BLOCK, dtype=jnp.float32)

    def process(payload):
        matrix, sweep_count = payload
        vectors = identity
        off_norms = []
        for sweep_index in range(MAXS):
            new_matrix, new_vectors = one_sweep(matrix, vectors)
            active = sweep_count > sweep_index
            matrix = jnp.where(active, new_matrix, matrix)
            vectors = jnp.where(active, new_vectors, vectors)
            off_norms.append(jnp.where(active, off_norm(new_matrix), jnp.float32(0.0)))
        return (root_factor(matrix, vectors), jnp.stack(off_norms))
    factors, all_norms = lax.map(process, (blocks_flat, sweeps_flat))
    off_max = lax.optimization_barrier(jnp.max(all_norms, axis=0))

    def apply_one(payload):
        factor, gradient = payload
        product = jnp.dot(factor.astype(jnp.float32), gradient.astype(jnp.float32), precision=highest)
        return product.astype(jnp.bfloat16)
    grads_flat = gradients.reshape(N_GRP * ROWB, BLOCK, FF)
    updates = lax.map(apply_one, (factors, grads_flat)).reshape(N_GRP, ROWB, BLOCK, FF)
    return (updates, off_max)
```

```python
import jax
import jax.numpy as jnp
from jax import lax
from jax.experimental import pallas as pl
from jax.experimental.pallas import tpu as pltpu
from jax.sharding import Mesh
from jax.sharding import PartitionSpec as P

MAXS = 2
SIZE = 512
W = 128
PAIRINGS = ((0, 1, 2, 3), (0, 2, 1, 3), (0, 3, 1, 2))
DAMPING = 0.01
SERIES_LIMIT = 1e-4
bf16 = jnp.bfloat16
f32 = jnp.float32


def halves(x):
    high = x.astype(bf16)
    low = (x - high.astype(f32)).astype(bf16)
    return high, low


def dot3(left, right):
    lh, ll = left
    rh, rl = right
    return jnp.dot(
        jnp.concatenate([lh, ll, lh], axis=1),
        jnp.concatenate([rh, rh, rl], axis=0),
        preferred_element_type=f32,
    )


def thirds(x):
    high, _ = halves(x)
    rest = x - high.astype(f32)
    middle, low = halves(rest)
    return high, middle, low


def dot6(left, right):
    a, b, c = thirds(left)
    x, y, z = thirds(right)
    return jnp.dot(
        jnp.concatenate([a, a, b, b, a, c], axis=1),
        jnp.concatenate([x, y, x, y, z, x], axis=0),
        preferred_element_type=f32,
    )


def beside(x, y):
    return tuple(jnp.concatenate([a, b], axis=1) for a, b in zip(x, y))


def angles_of(coupling, lower, upper):
    difference = upper - lower
    total = upper + lower
    bottom = difference * difference + 4.0 * coupling * coupling + DAMPING * (total * total)
    return coupling * difference / bottom


def span(member):
    return slice(member * W, member * W + W)


def eye(size):
    return lax.broadcasted_iota(jnp.int32, (size, size), 0) == lax.broadcasted_iota(
        jnp.int32, (size, size), 1
    )


def series_half(a, at, check):
    ah, th = halves(a), halves(at)
    x = 0.25 * dot3(ah, th)
    xh = halves(x)
    both = dot3(xh, beside(xh, ah))
    x2, b1 = both[:, :W], a - both[:, W:]
    x2h = halves(x2)
    both = dot3(x2h, beside(x2h, halves(b1)))
    x4, b2 = both[:, :W], b1 + both[:, W:]
    t = b2 + dot3(halves(x4), halves(b2))
    part = x4 * x4
    part = sum(part[8 * i : 8 * i + 8] for i in range(W // 8))
    check[...] += part
    tp = halves(t)
    return t, dot3(tp, th), dot3(th, tp)


def newton_half(a, at):
    one = jnp.where(eye(W), 1.0, 0.0).astype(f32)
    s = one + 0.25 * dot6(a, at)
    norm = jnp.max(jnp.sum(jnp.abs(s), axis=1, keepdims=True), axis=0, keepdims=True)

    def step(_, y):
        return dot6(y, 2.0 * one - dot6(s, y))

    y = lax.fori_loop(0, 14, step, one * (2.0 / (1.0 + norm)))
    t = dot6(y, a)
    return t, dot6(t, at), dot6(at, t)


def one_round(m, v, rot, check, pairing, exact):
    pairs = (pairing[:2], pairing[2:])
    diagonal = eye(W)
    one = jnp.where(diagonal, 1.0, 0.0).astype(f32)
    rs, rts = [], []
    for p, q in pairs:
        dp = jnp.where(diagonal, m[span(p), span(p)], 0.0)
        dq = jnp.where(diagonal, m[span(q), span(q)], 0.0)
        row_p, row_q = (jnp.sum(d, axis=0, keepdims=True) for d in (dp, dq))
        col_p, col_q = (jnp.sum(d, axis=1, keepdims=True) for d in (dp, dq))
        a = angles_of(m[span(p), span(q)], col_p, row_q)
        at = angles_of(m[span(q), span(p)], row_p, col_q)
        t, tat, att = newton_half(a, at) if exact else series_half(a, at, check)
        tt = t.T
        r00, r11 = one - 0.5 * tat, one - 0.5 * att
        rs.append(halves(jnp.concatenate(
            [jnp.concatenate([r00, t], axis=1), jnp.concatenate([-tt, r11], axis=1)], axis=0)))
        rts.append(halves(jnp.concatenate(
            [jnp.concatenate([r00, -t], axis=1), jnp.concatenate([tt, r11], axis=1)], axis=0)))

    def load(ref, rows, cols):
        return jnp.concatenate(
            [jnp.concatenate([ref[span(i), span(j)] for j in cols], axis=1) for i in rows], axis=0)

    def store(ref, rows, cols, value):
        for x, i in enumerate(rows):
            for y, j in enumerate(cols):
                ref[span(i), span(j)] = value[x * W : x * W + W, y * W : y * W + W]

    for x, y in ((0, 1), (0, 0), (1, 1)):
        rows, cols = pairs[x], pairs[y]
        g = dot3(halves(load(m, rows, cols)), rs[y])
        new = dot3(rts[x], halves(g))
        store(m, rows, cols, new)
        if x != y:
            store(m, cols, rows, new.T)
    for h, cols in enumerate(pairs):
        for i in range(4):
            new = dot3(halves(load(v, (i,), cols)), rs[h])
            store(v, (i,), cols, new)


def roots_kernel(run_ref, stat_ref, factor_ref, peaks_ref, m, v, check, norms):
    slot = pl.program_id(0)
    sweeps = run_ref[slot]

    @pl.when(slot == 0)
    def _():
        peaks_ref[...] = jnp.zeros_like(peaks_ref)

    def start():
        m[...] = stat_ref[0]
        v[...] = jnp.where(eye(SIZE), 1.0, 0.0).astype(f32)
        check[...] = jnp.zeros_like(check)
        norms[...] = jnp.zeros_like(norms)

    def all_sweeps(exact):
        def sweep(s, carry):
            for pairing in PAIRINGS:
                one_round(m, v, None, check, pairing, exact)
            square = m[...] * m[...]
            off = jnp.sum(jnp.where(eye(SIZE), 0.0, square), axis=0, keepdims=True)
            whole = jnp.sum(square, axis=0, keepdims=True)
            off = jnp.sum(off, axis=1, keepdims=True)
            whole = jnp.sum(whole, axis=1, keepdims=True)
            here = lax.broadcasted_iota(jnp.int32, (8, W), 0) == s
            norms[...] = jnp.where(here, jnp.sqrt(off / whole), norms[...])
            return carry
        lax.fori_loop(0, sweeps, sweep, 0)

    @pl.when(sweeps > 0)
    def _():
        start()
        all_sweeps(False)
        fine = jnp.sum(check[...]) <= SERIES_LIMIT

        @pl.when(jnp.logical_not(fine))
        def _():
            start()
            all_sweeps(True)

        square = jnp.where(eye(SIZE), m[...], 0.0)
        scale = jnp.sum(square, axis=0, keepdims=True)
        scale = lax.rsqrt(jnp.sqrt(scale))
        left = halves(v[...] * scale)
        right = halves(v[...])
        for i in range(4):
            lh, ll = (part[span(i)] for part in left)
            value = lax.dot_general(
                jnp.concatenate([lh, ll, lh], axis=1),
                jnp.concatenate([right[0], right[0], right[1]], axis=1),
                (((1,), (1,)), ((), ())),
                preferred_element_type=f32,
            )
            factor_ref[0, span(i)] = value.astype(bf16)
        peaks_ref[...] = jnp.maximum(peaks_ref[...], norms[...])

    @pl.when(sweeps == 0)
    def _():
        factor_ref[...] = jnp.zeros_like(factor_ref)


def roots(run, statistics):
    slots = statistics.shape[0]
    return pl.pallas_call(
        roots_kernel,
        grid_spec=pltpu.PrefetchScalarGridSpec(
            num_scalar_prefetch=1,
            grid=(slots,),
            in_specs=[pl.BlockSpec((1, SIZE, SIZE), lambda i, run: (i, 0, 0))],
            out_specs=[
                pl.BlockSpec((1, SIZE, SIZE), lambda i, run: (i, 0, 0)),
                pl.BlockSpec((8, W), lambda i, run: (0, 0)),
            ],
            scratch_shapes=[
                pltpu.VMEM((SIZE, SIZE), f32),
                pltpu.VMEM((SIZE, SIZE), f32),
                pltpu.VMEM((8, W), f32),
                pltpu.VMEM((8, W), f32),
            ],
        ),
        out_shape=[
            jax.ShapeDtypeStruct((slots, SIZE, SIZE), bf16),
            jax.ShapeDtypeStruct((8, W), f32),
        ],
        compiler_params=pltpu.CompilerParams(dimension_semantics=("arbitrary",)),
    )(run, statistics)


BLK = ("blk_0", "blk_1", "blk_2")
BLK_GRP = ("blk_0", "blk_1", "blk_2", "grp")


def per_device(statistics, gradients, live_counts, slot_row, sweeps):
    slot_count = statistics.shape[1]
    row_count = gradients.shape[1]
    blk_rank = lax.axis_index(BLK)
    own_live = lax.dynamic_index_in_dim(live_counts[0], blk_rank, 0, keepdims=False)
    run = jnp.where(lax.iota(jnp.int32, slot_count) < own_live, sweeps[0], 0)
    factors, peaks = roots(run, statistics[0])
    off_max = peaks[:MAXS, 0]
    for axis in BLK_GRP:
        off_max = lax.pmax(off_max, axis)
    gathered = lax.all_gather(factors, BLK, axis=0, tiled=True)
    slot_total = gathered.shape[0]
    slot_ids = lax.iota(jnp.int32, slot_total)
    row_ids = lax.iota(jnp.int32, row_count)
    is_live = slot_ids % slot_count < jnp.repeat(live_counts[0], slot_count)
    matches = (slot_row[0][None, :] == row_ids[:, None]) & is_live[None, :]
    slot_of = jnp.sum(jnp.where(matches, slot_ids[None, :], 0), axis=1)
    chosen = jnp.take(gathered, slot_of, axis=0)
    updates = jnp.einsum("kij,kjc->kic", chosen, gradients[0], preferred_element_type=jnp.float32)
    return (updates.astype(jnp.bfloat16)[None], off_max)


def solution(mesh):
    split = Mesh(
        mesh.devices.reshape(4, 4, 2, mesh.shape["grp"]), ("blk_0", "blk_1", "blk_2", "grp")
    )
    return jax.shard_map(
        per_device,
        mesh=split,
        in_specs=(
            P("grp", BLK, None, None),
            P("grp", None, None, BLK),
            P("grp", None),
            P("grp", None),
            P("grp", BLK),
        ),
        out_specs=(P("grp", None, None, BLK), P()),
        check_vma=False,
    )
```

```python
import jax
import jax.numpy as jnp
from jax import lax
from jax.experimental import pallas as pl
from jax.experimental.pallas import tpu as pltpu
from jax.sharding import Mesh
from jax.sharding import PartitionSpec as P

MAXS = 2
SIZE = 512
W = 128
PAIRINGS = ((0, 1, 2, 3), (0, 2, 1, 3), (0, 3, 1, 2))
DAMPING = 0.01
SERIES_LIMIT = 1e-4
OFF_LEAST = 0.1
SPINE_LEAST = 0.1
bf16 = jnp.bfloat16
f32 = jnp.float32


def halves(x):
    high = x.astype(bf16)
    low = (x - high.astype(f32)).astype(bf16)
    return high, low


def dot1(left, right):
    return jnp.dot(left.astype(bf16), right.astype(bf16), preferred_element_type=f32)


def dot2(left, right):
    right = right.astype(bf16)
    return jnp.dot(
        jnp.concatenate(halves(left), axis=1),
        jnp.concatenate([right, right], axis=0),
        preferred_element_type=f32,
    )


def thirds(x):
    high, _ = halves(x)
    rest = x - high.astype(f32)
    middle, low = halves(rest)
    return high, middle, low


def dot6(left, right):
    a, b, c = thirds(left)
    x, y, z = thirds(right)
    return jnp.dot(
        jnp.concatenate([a, a, b, b, a, c], axis=1),
        jnp.concatenate([x, y, x, y, z, x], axis=0),
        preferred_element_type=f32,
    )


def angles_of(coupling, lower, upper):
    difference = upper - lower
    total = upper + lower
    bottom = difference * difference + 4.0 * coupling * coupling + DAMPING * (total * total)
    return coupling * difference / bottom


def span(member):
    return slice(member * W, member * W + W)


def eye(size):
    return lax.broadcasted_iota(jnp.int32, (size, size), 0) == lax.broadcasted_iota(
        jnp.int32, (size, size), 1
    )


def series_half(a, at, check):
    x = 0.25 * dot1(a, at)
    both = dot1(x, jnp.concatenate([x, a], axis=1))
    x2, b1 = both[:, :W], a - both[:, W:]
    both = dot1(x2, jnp.concatenate([x2, b1], axis=1))
    x4, b2 = both[:, :W], b1 + both[:, W:]
    t = b2 + dot1(x4, b2)
    part = x4 * x4
    check[...] += sum(part[8 * i : 8 * i + 8] for i in range(W // 8))
    return t, dot1(t, at), dot1(at, t)


def newton_half(a, at):
    one = jnp.where(eye(W), 1.0, 0.0).astype(f32)
    s = one + 0.25 * dot6(a, at)
    norm = jnp.max(jnp.sum(jnp.abs(s), axis=1, keepdims=True), axis=0, keepdims=True)

    def step(_, y):
        return dot6(y, 2.0 * one - dot6(s, y))

    y = lax.fori_loop(0, 14, step, one * (2.0 / (1.0 + norm)))
    t = dot6(y, a)
    return t, dot6(t, at), dot6(at, t)


def one_round(m, v, check, pairing, exact):
    pairs = (pairing[:2], pairing[2:])
    diagonal = eye(W)
    mul, mul_v = (dot6, dot6) if exact else (dot1, dot2)
    keep = (lambda x: x) if exact else (lambda x: x.astype(bf16))
    rs, rts = [], []
    for p, q in pairs:
        dp = jnp.where(diagonal, m[span(p), span(p)], 0.0)
        dq = jnp.where(diagonal, m[span(q), span(q)], 0.0)
        row_p, row_q = (jnp.sum(d, axis=0, keepdims=True) for d in (dp, dq))
        col_p, col_q = (jnp.sum(d, axis=1, keepdims=True) for d in (dp, dq))
        a = angles_of(m[span(p), span(q)], col_p, row_q)
        at = angles_of(m[span(q), span(p)], row_p, col_q)
        t, tat, att = newton_half(a, at) if exact else series_half(a, at, check)
        tt = t.T
        r00, r11 = -0.5 * tat, -0.5 * att
        rs.append(keep(jnp.concatenate(
            [jnp.concatenate([r00, t], axis=1), jnp.concatenate([-tt, r11], axis=1)], axis=0)))
        rts.append(keep(jnp.concatenate(
            [jnp.concatenate([r00, -t], axis=1), jnp.concatenate([tt, r11], axis=1)], axis=0)))

    def load(ref, rows, cols):
        return jnp.concatenate(
            [jnp.concatenate([ref[span(i), span(j)] for j in cols], axis=1) for i in rows], axis=0)

    def store(ref, rows, cols, value):
        for x, i in enumerate(rows):
            for y, j in enumerate(cols):
                ref[span(i), span(j)] = value[x * W : x * W + W, y * W : y * W + W]

    for x, y in ((0, 1), (0, 0), (1, 1)):
        rows, cols = pairs[x], pairs[y]
        old = load(m, rows, cols)
        g = old + mul(old, rs[y])
        new = g + mul(rts[x], g)
        store(m, rows, cols, new)
        if x != y:
            store(m, cols, rows, new.T)
    for h, cols in enumerate(pairs):
        old = load(v, range(4), cols)
        store(v, range(4), cols, old + mul_v(old, rs[h]))


def off_of(ref):
    square = ref[...] * ref[...]
    off = jnp.sum(jnp.where(eye(SIZE), 0.0, square), axis=0, keepdims=True)
    whole = jnp.sum(square, axis=0, keepdims=True)
    return jnp.sqrt(jnp.sum(off, axis=1, keepdims=True) / jnp.sum(whole, axis=1, keepdims=True))


def spine_of(value):
    size = value.shape[0]
    return jnp.sum(jnp.where(eye(size), value, 0.0), axis=0, keepdims=True)


HALF = SIZE // 2
STRIPS = 32
ROWS = SIZE // STRIPS
BLOCKS = 16
SHIFTS = (0, 1, 3, 2)
PART = 8
TOGETHER = 4
WIDE = 2 * HALF + W
BLK = ("x", "z", "c")


def roots_kernel(live_ref, sweeps_ref, stat_ref, out_ref, m, v, check, norms, peaks, before, extra):
    slot = pl.program_id(0)
    live = live_ref[0, lax.axis_index(BLK)]
    sweeps = jnp.where(slot < live, sweeps_ref[0, slot], 0)
    lane = lax.broadcasted_iota(jnp.int32, (8, W), 1)

    @pl.when(slot == 0)
    def _():
        peaks[...] = jnp.zeros_like(peaks)
        extra[...] = jnp.zeros_like(extra)
        out_ref[...] = jnp.zeros_like(out_ref)

    def start():
        m[...] = stat_ref[0, 0]
        v[...] = jnp.where(eye(SIZE), 1.0, 0.0).astype(f32)
        check[...] = jnp.zeros_like(check)
        norms[...] = jnp.zeros_like(norms)
        before[...] = jnp.broadcast_to(off_of(m), before.shape)

    def all_sweeps(exact):
        def sweep(s, carry):
            for pairing in PAIRINGS:
                one_round(m, v, check, pairing, exact)
            off = off_of(m)
            norms[...] = jnp.where(lane == s, off, norms[...])
            check[...] += jnp.where(off >= OFF_LEAST * before[...], 0.0, 1.0)
            return carry

        lax.fori_loop(0, sweeps, sweep, 0)

    @pl.when(sweeps > 0)
    def _():
        start()
        all_sweeps(False)
        shrunk = jnp.where(spine_of(m[...]) >= SPINE_LEAST * spine_of(stat_ref[0, 0]), 0.0, 1.0)
        fine = jnp.sum(check[...]) + jnp.sum(shrunk) <= SERIES_LIMIT

        @pl.when(jnp.logical_not(fine))
        def _():
            start()
            all_sweeps(True)

        scale = lax.rsqrt(jnp.sqrt(spine_of(m[...])))

        def piece(rows, others):
            lh, ll = halves(v[rows] * scale)
            rh, rl = halves(v[others])
            return lax.dot_general(
                jnp.concatenate([lh, ll, lh], axis=1),
                jnp.concatenate([rh, rh, rl], axis=1),
                (((1,), (1,)), ((), ())),
                preferred_element_type=f32,
            )

        top, low = slice(0, HALF), slice(HALF, SIZE)
        corner = piece(low, low)
        upper = lax.broadcasted_iota(jnp.int32, (HALF, HALF), 0) <= lax.broadcasted_iota(
            jnp.int32, (HALF, HALF), 1
        )
        folded = jnp.where(upper, piece(top, top), corner).astype(bf16)
        beyond = piece(top, low).astype(bf16)
        spine = spine_of(corner)
        for j in range(2):

            @pl.when(slot == j)
            def _():
                cols = slice(j * HALF, j * HALF + HALF)
                out_ref[: STRIPS // 2, :, cols] = folded.reshape(STRIPS // 2, ROWS, HALF)
                out_ref[STRIPS // 2 :, :, cols] = beyond.reshape(STRIPS // 2, ROWS, HALF)
                extra[2 * j : 2 * j + 1] = spine[:, :W]
                extra[2 * j + 1 : 2 * j + 2] = spine[:, W:]

        peaks[...] = jnp.maximum(peaks[...], norms[...])

    @pl.when(slot == 1)
    def _():
        for i, part in enumerate(thirds(peaks[0:1])):
            extra[4 + i : 5 + i] = part.astype(f32)
        tile = extra[...].astype(bf16)
        for d in range(STRIPS):
            out_ref[d, :, 2 * HALF :] = tile


def roots(live_counts, sweeps, statistics):
    slots = statistics.shape[1]
    return pl.pallas_call(
        roots_kernel,
        grid_spec=pltpu.PrefetchScalarGridSpec(
            num_scalar_prefetch=2,
            grid=(slots,),
            in_specs=[pl.BlockSpec((1, 1, SIZE, SIZE), lambda i, *_: (0, i, 0, 0))],
            out_specs=pl.BlockSpec((STRIPS, ROWS, WIDE), lambda i, *_: (0, 0, 0)),
            scratch_shapes=[
                pltpu.VMEM((SIZE, SIZE), f32),
                pltpu.VMEM((SIZE, SIZE), f32),
                pltpu.VMEM((8, W), f32),
                pltpu.VMEM((8, W), f32),
                pltpu.VMEM((8, W), f32),
                pltpu.VMEM((8, W), f32),
                pltpu.VMEM((ROWS, W), f32),
            ],
        ),
        out_shape=jax.ShapeDtypeStruct((STRIPS, ROWS, WIDE), bf16),
        compiler_params=pltpu.CompilerParams(dimension_semantics=("arbitrary",)),
        name="roots",
    )(live_counts, sweeps, statistics)


def select_kernel(live_ref, row_ref, got_ref, *refs):
    piece_ref, spine_ref, peak_ref, table = refs

    def note(s, carry):
        @pl.when(s % 2 < live_ref[0, s // 2])
        def _():
            table[row_ref[0, s]] = s

        return carry

    lax.fori_loop(0, 2 * STRIPS, note, 0)
    peak = jnp.zeros((1, W), f32)
    for d in range(STRIPS):
        parts = got_ref[d, :, 2 * HALF :].astype(f32)
        peak = jnp.maximum(peak, parts[4:5] + parts[5:6] + parts[6:7])
    peak_ref[...] = jnp.broadcast_to(peak, (8, W))
    for k in range(BLOCKS):
        s = table[k]
        source = s // 2
        second = s % 2 == 1
        strip = jnp.where(second, got_ref[source, :, HALF : 2 * HALF], got_ref[source, :, :HALF])
        piece_ref[k] = strip
        parts = got_ref[source, :, 2 * HALF :].astype(f32)
        spine_ref[2 * k : 2 * k + 2] = jnp.where(second, parts[2:4], parts[0:2])


def select(live_counts, slot_row, got):
    whole = pl.BlockSpec(memory_space=pltpu.VMEM)
    scalars = pl.BlockSpec(memory_space=pltpu.SMEM)
    return pl.pallas_call(
        select_kernel,
        in_specs=[scalars, scalars, whole],
        out_specs=[whole] * 3,
        out_shape=[
            jax.ShapeDtypeStruct((BLOCKS, ROWS, HALF), bf16),
            jax.ShapeDtypeStruct((2 * BLOCKS, W), f32),
            jax.ShapeDtypeStruct((8, W), f32),
        ],
        scratch_shapes=[pltpu.SMEM((BLOCKS,), jnp.int32)],
        name="select",
    )(live_counts, slot_row, got)


def apply_kernel(*refs):
    pieces = refs[:8]
    spine_ref, grad_ref, out_ref, packed, full, sems = refs[8:]
    k = pl.program_id(0)
    x, z, c = (lax.axis_index(name) for name in BLK)

    def copies(part):
        for i, piece in enumerate(pieces):
            core, step = (c, 1 - c)[i // 4], i % 4
            for other in range(4):
                near, far = SHIFTS[other], SHIFTS[step]
                dx = far + core * (near - far)
                dz = near + core * (far - near)
                chip = ((x - dx + 4) % 4) * 4 + (z - dz + 4) % 4
                strip = chip * 2 + core
                yield pltpu.make_async_copy(
                    piece.at[other, pl.ds(part * PART, PART)],
                    packed.at[
                        pl.ds(part * PART, PART),
                        pl.ds(pl.multiple_of(strip * ROWS, ROWS), ROWS),
                    ],
                    sems.at[part, i * 4 + other],
                )

    @pl.when(k == 0)
    def _():
        for part in range(BLOCKS // PART):
            for copy in copies(part):
                copy.start()

    for part in range(BLOCKS // PART):

        @pl.when(k == part * PART // TOGETHER)
        def _():
            for copy in copies(part):
                copy.wait()

    one = jnp.where(eye(HALF), 1.0, 0.0).astype(bf16)
    across = lax.broadcasted_iota(jnp.int32, (HALF, HALF), 1)
    down = lax.broadcasted_iota(jnp.int32, (HALF, HALF), 0)

    def turned(x):
        return lax.dot_general(
            one, x, (((1,), (1,)), ((), ())), preferred_element_type=f32
        ).astype(bf16)

    for j in range(TOGETHER):
        block = k * TOGETHER + j
        folded, beyond = packed[block, :HALF], packed[block, HALF:]
        mirrored = turned(folded)
        pair = spine_ref[pl.ds(2 * block, 2)]
        spine = jnp.concatenate([pair[0:1], pair[1:2]], axis=1).astype(bf16)
        first = jnp.where(across >= down, folded, mirrored)
        last = jnp.where(across < down, folded, mirrored)
        last = jnp.where(across == down, jnp.broadcast_to(spine, (HALF, HALF)), last)
        full[j, :HALF, :HALF] = first
        full[j, :HALF, HALF:] = beyond
        full[j, HALF:, :HALF] = turned(beyond)
        full[j, HALF:, HALF:] = last
    for j in range(TOGETHER):
        value = jnp.dot(grad_ref[0, j], full[j], preferred_element_type=f32)
        out_ref[0, j] = value.astype(bf16)


def apply(pieces, spine, gradients):
    cols = gradients.shape[-1]
    block = pl.BlockSpec((1, TOGETHER, cols, SIZE), lambda k: (0, k, 0, 0))
    anywhere = pl.BlockSpec(memory_space=pl.ANY)
    turned = jnp.swapaxes(gradients, 2, 3)
    updates = pl.pallas_call(
        apply_kernel,
        grid=(BLOCKS // TOGETHER,),
        in_specs=[anywhere] * 8 + [pl.BlockSpec((2 * BLOCKS, W), lambda k: (0, 0)), block],
        out_specs=block,
        out_shape=jax.ShapeDtypeStruct(turned.shape, bf16),
        scratch_shapes=[
            pltpu.VMEM((BLOCKS, SIZE, HALF), bf16),
            pltpu.VMEM((TOGETHER, SIZE, SIZE), bf16),
            pltpu.SemaphoreType.DMA((BLOCKS // PART, 32)),
        ],
        compiler_params=pltpu.CompilerParams(dimension_semantics=("arbitrary",)),
        name="apply",
    )(*pieces, spine, turned)
    return jnp.swapaxes(updates, 2, 3)


def shift(value, axis, by):
    return lax.ppermute(value, axis, [(i, (i + by) % 4) for i in range(4)])


def swap_cores(value):
    return lax.ppermute(value, "c", [(0, 1), (1, 0)])


def crossed(value, stage, by):
    pairs = []
    for x in range(4):
        for z in range(4):
            for c in range(2):
                along_x = stage != c
                to = ((x + by) % 4, z) if along_x else (x, (z + by) % 4)
                pairs.append(((x * 4 + z) * 2 + c, (to[0] * 4 + to[1]) * 2 + c))
    return lax.ppermute(value, BLK, pairs)


def gather_pieces(piece):
    line = jnp.stack([piece] + [crossed(piece, 0, by) for by in SHIFTS[1:]])
    own = [line] + [crossed(line, 1, by) for by in SHIFTS[1:]]
    return own + [swap_cores(value) for value in own]


def per_device(statistics, gradients, live_counts, slot_row, sweeps):
    strips = roots(live_counts, sweeps, statistics)
    got = lax.all_to_all(strips, BLK, 0, 0, tiled=True)
    piece, spine, peak = select(live_counts, slot_row, got)
    peaks = [peak] + [shift(peak, "grp", by) for by in (1, 2, 3)]
    updates = apply(gather_pieces(piece), spine, gradients)
    off_max = jnp.max(jnp.stack([value[0, :MAXS] for value in peaks]), axis=0)
    return (updates, off_max)


def solution(mesh):
    split = Mesh(mesh.devices.reshape(4, 4, 2, mesh.shape["grp"]), BLK + ("grp",))
    return jax.shard_map(
        per_device,
        mesh=split,
        in_specs=(
            P("grp", BLK, None, None),
            P("grp", None, None, BLK),
            P("grp", None),
            P("grp", None),
            P("grp", BLK),
        ),
        out_specs=(P("grp", None, None, BLK), P()),
        check_vma=False,
    )
```

```python
import jax
import jax.numpy as jnp
from jax import lax
from jax.experimental import pallas as pl
from jax.experimental.pallas import tpu as pltpu
from jax.sharding import Mesh
from jax.sharding import PartitionSpec as P

MAXS = 2
SIZE = 512
W = 128
PAIRINGS = ((0, 1, 2, 3), (0, 2, 1, 3), (0, 3, 1, 2))
DAMPING = 0.01
SERIES_LIMIT = 1e-4
OFF_LEAST = 0.1
SPINE_LEAST = 0.1
bf16 = jnp.bfloat16
f32 = jnp.float32


def halves(x):
    high = x.astype(bf16)
    low = (x - high.astype(f32)).astype(bf16)
    return high, low


def dot1(left, right):
    return jnp.dot(left.astype(bf16), right.astype(bf16), preferred_element_type=f32)


def dot2(left, right):
    right = right.astype(bf16)
    return jnp.dot(
        jnp.concatenate(halves(left), axis=1),
        jnp.concatenate([right, right], axis=0),
        preferred_element_type=f32,
    )


def thirds(x):
    high, _ = halves(x)
    rest = x - high.astype(f32)
    middle, low = halves(rest)
    return high, middle, low


def dot6(left, right):
    a, b, c = thirds(left)
    x, y, z = thirds(right)
    return jnp.dot(
        jnp.concatenate([a, a, b, b, a, c], axis=1),
        jnp.concatenate([x, y, x, y, z, x], axis=0),
        preferred_element_type=f32,
    )


def angles_of(coupling, lower, upper):
    difference = upper - lower
    total = upper + lower
    bottom = difference * difference + 4.0 * coupling * coupling + DAMPING * (total * total)
    return coupling * difference / bottom


def span(member):
    return slice(member * W, member * W + W)


def eye(size):
    return lax.broadcasted_iota(jnp.int32, (size, size), 0) == lax.broadcasted_iota(
        jnp.int32, (size, size), 1
    )


def series_halves(items, checks):
    sides = [pair for a, at in items for pair in ((a, at), (at, a))]
    x1 = [0.25 * dot1(a, at) for a, at in sides]
    both = [dot1(x, jnp.concatenate([x, a], axis=1)) for x, (a, _) in zip(x1, sides)]
    x2 = [y[:, :W] for y in both]
    b1 = [a - y[:, W:] for y, (a, _) in zip(both, sides)]
    three = [dot1(y, jnp.concatenate([y, b, x], axis=1)) for y, b, x in zip(x2, b1, x1)]
    x4 = [y[:, :W] for y in three]
    b2 = [b + y[:, W : 2 * W] for b, y in zip(b1, three)]
    p0 = [y - x - z[:, 2 * W :] for x, y, z in zip(x1, x2, three)]
    last = [dot1(y, jnp.concatenate([b, p], axis=1)) for y, b, p in zip(x4, b2, p0)]
    ts = [b + y[:, :W] for b, y in zip(b2, last)]
    rs = [2.0 * (p + x + y[:, W:]) for p, x, y in zip(p0, x4, last)]
    for i, check in enumerate(checks):
        part = x4[2 * i] * x4[2 * i]
        check[...] += sum(part[8 * j : 8 * j + 8] for j in range(W // 8))
    return [(ts[2 * i], ts[2 * i + 1], rs[2 * i], rs[2 * i + 1]) for i in range(len(items))]


def newton_half(a, at):
    one = jnp.where(eye(W), 1.0, 0.0).astype(f32)
    s = one + 0.25 * dot6(a, at)
    norm = jnp.max(jnp.sum(jnp.abs(s), axis=1, keepdims=True), axis=0, keepdims=True)

    def step(_, y):
        return dot6(y, 2.0 * one - dot6(s, y))

    y = lax.fori_loop(0, 14, step, one * (2.0 / (1.0 + norm)))
    t = dot6(y, a)
    return t, t.T, -0.5 * dot6(t, at), -0.5 * dot6(at, t)


def one_round(states, pairing, exact):
    pairs = (pairing[:2], pairing[2:])
    diagonal = eye(W)
    mul, mul_v = (dot6, dot6) if exact else (dot1, dot2)
    keep = (lambda x: x) if exact else (lambda x: x.astype(bf16))
    items, checks = [], []
    for m, _, check in states:
        for p, q in pairs:
            dp = jnp.where(diagonal, m[span(p), span(p)], 0.0)
            dq = jnp.where(diagonal, m[span(q), span(q)], 0.0)
            row_p, row_q = (jnp.sum(d, axis=0, keepdims=True) for d in (dp, dq))
            col_p, col_q = (jnp.sum(d, axis=1, keepdims=True) for d in (dp, dq))
            a = angles_of(m[span(p), span(q)], col_p, row_q)
            at = angles_of(m[span(q), span(p)], row_p, col_q)
            items.append((a, at))
            checks.append(check)
    if exact:
        parts = [newton_half(*item) for item in items]
    else:
        parts = series_halves(items, checks)
    rs, rts = [], []
    for t, tt, r00, r11 in parts:
        rs.append(keep(jnp.concatenate(
            [jnp.concatenate([r00, t], axis=1), jnp.concatenate([-tt, r11], axis=1)], axis=0)))
        rts.append(keep(jnp.concatenate(
            [jnp.concatenate([r00, -t], axis=1), jnp.concatenate([tt, r11], axis=1)], axis=0)))

    def load(ref, rows, cols):
        return jnp.concatenate(
            [jnp.concatenate([ref[span(i), span(j)] for j in cols], axis=1) for i in rows], axis=0)

    def store(ref, rows, cols, value):
        for x, i in enumerate(rows):
            for y, j in enumerate(cols):
                ref[span(i), span(j)] = value[x * W : x * W + W, y * W : y * W + W]

    todo = [(i, x, y) for x, y in ((0, 1), (0, 0), (1, 1)) for i in range(len(states))]
    olds = [load(states[i][0], pairs[x], pairs[y]) for i, x, y in todo]
    gs = [old + mul(old, rs[2 * i + y]) for old, (i, x, y) in zip(olds, todo)]
    news = [g + mul(rts[2 * i + x], g) for g, (i, x, y) in zip(gs, todo)]
    for new, (i, x, y) in zip(news, todo):
        store(states[i][0], pairs[x], pairs[y], new)
        if x != y:
            store(states[i][0], pairs[y], pairs[x], new.T)
    for i, (_, v, _) in enumerate(states):
        for h, cols in enumerate(pairs):
            old = load(v, range(4), cols)
            store(v, range(4), cols, old + mul_v(old, rs[2 * i + h]))


def off_of(ref):
    square = ref[...] * ref[...]
    off = jnp.sum(jnp.where(eye(SIZE), 0.0, square), axis=0, keepdims=True)
    whole = jnp.sum(square, axis=0, keepdims=True)
    return jnp.sqrt(jnp.sum(off, axis=1, keepdims=True) / jnp.sum(whole, axis=1, keepdims=True))


def spine_of(value):
    size = value.shape[0]
    return jnp.sum(jnp.where(eye(size), value, 0.0), axis=0, keepdims=True)


HALF = SIZE // 2
STRIPS = 32
ROWS = SIZE // STRIPS
BLOCKS = 16
SHIFTS = (0, 1, 3, 2)
PART = 8
TOGETHER = 4
WIDE = 2 * HALF + W
BLK = ("x", "z", "c")


def roots_kernel(live_ref, sweeps_ref, stat_ref, out_ref, m, v, check, norms, before, extra):
    live = live_ref[0, lax.axis_index(BLK)]
    counts = [jnp.where(j < live, sweeps_ref[0, j], 0) for j in range(2)]
    lane = lax.broadcasted_iota(jnp.int32, (8, W), 1)
    norms[...] = jnp.zeros_like(norms)
    extra[...] = jnp.zeros_like(extra)

    def start(slot):
        m[slot] = stat_ref[0, slot]
        v[slot] = jnp.where(eye(SIZE), 1.0, 0.0).astype(f32)
        check[slot] = jnp.zeros((8, W), f32)
        norms[slot] = jnp.zeros((8, W), f32)
        before[slot] = jnp.broadcast_to(off_of(m.at[slot]), (8, W))

    def sweep_of(slots, exact):
        def sweep(s, carry):
            for pairing in PAIRINGS:
                one_round([(m.at[j], v.at[j], check.at[j]) for j in slots], pairing, exact)
            for j in slots:
                off = off_of(m.at[j])
                norms[j] = jnp.where(lane == s, off, norms[j])
                check[j] += jnp.where(off >= OFF_LEAST * before[j], 0.0, 1.0)
            return carry

        return sweep

    for j in range(2):

        @pl.when(counts[j] > 0)
        def _():
            start(j)

        @pl.when(counts[j] == 0)
        def _():
            cols = slice(j * HALF, j * HALF + HALF)
            out_ref[:, :, cols] = jnp.zeros((STRIPS, ROWS, HALF), bf16)

    common = jnp.minimum(counts[0], counts[1])
    longer = jnp.where(counts[0] >= counts[1], 0, 1)
    lax.fori_loop(0, common, sweep_of((0, 1), False), 0)
    lax.fori_loop(common, jnp.maximum(counts[0], counts[1]), sweep_of((longer,), False), 0)

    def again(slot, carry):
        count = jnp.where(slot == 0, counts[0], counts[1])

        @pl.when(count > 0)
        def _():
            least = SPINE_LEAST * spine_of(stat_ref[0, slot])
            shrunk = jnp.where(spine_of(m[slot]) >= least, 0.0, 1.0)
            fine = jnp.sum(check[slot]) + jnp.sum(shrunk) <= SERIES_LIMIT

            @pl.when(jnp.logical_not(fine))
            def _():
                start(slot)
                lax.fori_loop(0, count, sweep_of((slot,), True), 0)

        return carry

    lax.fori_loop(0, 2, again, 0)
    top, low = slice(0, HALF), slice(HALF, SIZE)
    for j in range(2):

        @pl.when(counts[j] > 0)
        def _():
            scale = lax.rsqrt(jnp.sqrt(spine_of(m[j])))

            def piece(rows, others):
                lh, ll = halves(v[j, rows] * scale)
                rh, rl = halves(v[j, others])
                return lax.dot_general(
                    jnp.concatenate([lh, ll, lh], axis=1),
                    jnp.concatenate([rh, rh, rl], axis=1),
                    (((1,), (1,)), ((), ())),
                    preferred_element_type=f32,
                )

            corner = piece(low, low)
            upper = lax.broadcasted_iota(jnp.int32, (HALF, HALF), 0) <= lax.broadcasted_iota(
                jnp.int32, (HALF, HALF), 1
            )
            folded = jnp.where(upper, piece(top, top), corner).astype(bf16)
            beyond = piece(top, low).astype(bf16)
            spine = spine_of(corner)
            cols = slice(j * HALF, j * HALF + HALF)
            out_ref[: STRIPS // 2, :, cols] = folded.reshape(STRIPS // 2, ROWS, HALF)
            out_ref[STRIPS // 2 :, :, cols] = beyond.reshape(STRIPS // 2, ROWS, HALF)
            extra[2 * j : 2 * j + 1] = spine[:, :W]
            extra[2 * j + 1 : 2 * j + 2] = spine[:, W:]

    for i, part in enumerate(thirds(jnp.maximum(norms[0, 0:1], norms[1, 0:1]))):
        extra[4 + i : 5 + i] = part.astype(f32)
    tile = extra[...].astype(bf16)
    for d in range(STRIPS):
        out_ref[d, :, 2 * HALF :] = tile


def roots(live_counts, sweeps, statistics):
    slots = statistics.shape[1]
    whole = pl.BlockSpec(memory_space=pltpu.VMEM)
    scalars = pl.BlockSpec(memory_space=pltpu.SMEM)
    return pl.pallas_call(
        roots_kernel,
        in_specs=[scalars, scalars, whole],
        out_specs=whole,
        scratch_shapes=[
            pltpu.VMEM((slots, SIZE, SIZE), f32),
            pltpu.VMEM((slots, SIZE, SIZE), f32),
            pltpu.VMEM((slots, 8, W), f32),
            pltpu.VMEM((slots, 8, W), f32),
            pltpu.VMEM((slots, 8, W), f32),
            pltpu.VMEM((ROWS, W), f32),
        ],
        out_shape=jax.ShapeDtypeStruct((STRIPS, ROWS, WIDE), bf16),
        name="roots",
    )(live_counts, sweeps, statistics)


def select_kernel(live_ref, row_ref, got_ref, *refs):
    piece_ref, spine_ref, peak_ref, table = refs

    def note(s, carry):
        @pl.when(s % 2 < live_ref[0, s // 2])
        def _():
            table[row_ref[0, s]] = s

        return carry

    lax.fori_loop(0, 2 * STRIPS, note, 0)
    peak = jnp.zeros((1, W), f32)
    for d in range(STRIPS):
        parts = got_ref[d, :, 2 * HALF :].astype(f32)
        peak = jnp.maximum(peak, parts[4:5] + parts[5:6] + parts[6:7])
    peak_ref[...] = jnp.broadcast_to(peak, (8, W))
    for k in range(BLOCKS):
        s = table[k]
        source = s // 2
        second = s % 2 == 1
        strip = jnp.where(second, got_ref[source, :, HALF : 2 * HALF], got_ref[source, :, :HALF])
        piece_ref[k] = strip
        parts = got_ref[source, :, 2 * HALF :].astype(f32)
        spine_ref[2 * k : 2 * k + 2] = jnp.where(second, parts[2:4], parts[0:2])


def select(live_counts, slot_row, got):
    whole = pl.BlockSpec(memory_space=pltpu.VMEM)
    scalars = pl.BlockSpec(memory_space=pltpu.SMEM)
    return pl.pallas_call(
        select_kernel,
        in_specs=[scalars, scalars, whole],
        out_specs=[whole] * 3,
        out_shape=[
            jax.ShapeDtypeStruct((BLOCKS, ROWS, HALF), bf16),
            jax.ShapeDtypeStruct((2 * BLOCKS, W), f32),
            jax.ShapeDtypeStruct((8, W), f32),
        ],
        scratch_shapes=[pltpu.SMEM((BLOCKS,), jnp.int32)],
        name="select",
    )(live_counts, slot_row, got)


def apply_kernel(*refs):
    pieces = refs[:8]
    spine_ref, grad_ref, out_ref, packed, full, sems = refs[8:]
    k = pl.program_id(0)
    x, z, c = (lax.axis_index(name) for name in BLK)

    def copies(part):
        for i, piece in enumerate(pieces):
            core, step = (c, 1 - c)[i // 4], i % 4
            for other in range(4):
                near, far = SHIFTS[other], SHIFTS[step]
                dx = far + core * (near - far)
                dz = near + core * (far - near)
                chip = ((x - dx + 4) % 4) * 4 + (z - dz + 4) % 4
                strip = chip * 2 + core
                yield pltpu.make_async_copy(
                    piece.at[other, pl.ds(part * PART, PART)],
                    packed.at[
                        pl.ds(part * PART, PART),
                        pl.ds(pl.multiple_of(strip * ROWS, ROWS), ROWS),
                    ],
                    sems.at[part, i * 4 + other],
                )

    @pl.when(k == 0)
    def _():
        for part in range(BLOCKS // PART):
            for copy in copies(part):
                copy.start()

    for part in range(BLOCKS // PART):

        @pl.when(k == part * PART // TOGETHER)
        def _():
            for copy in copies(part):
                copy.wait()

    one = jnp.where(eye(HALF), 1.0, 0.0).astype(bf16)
    across = lax.broadcasted_iota(jnp.int32, (HALF, HALF), 1)
    down = lax.broadcasted_iota(jnp.int32, (HALF, HALF), 0)

    def turned(x):
        return lax.dot_general(
            one, x, (((1,), (1,)), ((), ())), preferred_element_type=f32
        ).astype(bf16)

    for j in range(TOGETHER):
        block = k * TOGETHER + j
        folded, beyond = packed[block, :HALF], packed[block, HALF:]
        mirrored = turned(folded)
        pair = spine_ref[pl.ds(2 * block, 2)]
        spine = jnp.concatenate([pair[0:1], pair[1:2]], axis=1).astype(bf16)
        first = jnp.where(across >= down, folded, mirrored)
        last = jnp.where(across < down, folded, mirrored)
        last = jnp.where(across == down, jnp.broadcast_to(spine, (HALF, HALF)), last)
        full[j, :HALF, :HALF] = first
        full[j, :HALF, HALF:] = beyond
        full[j, HALF:, :HALF] = turned(beyond)
        full[j, HALF:, HALF:] = last
    for j in range(TOGETHER):
        value = jnp.dot(grad_ref[0, j], full[j], preferred_element_type=f32)
        out_ref[0, j] = value.astype(bf16)


def apply(pieces, spine, gradients):
    cols = gradients.shape[-1]
    block = pl.BlockSpec((1, TOGETHER, cols, SIZE), lambda k: (0, k, 0, 0))
    anywhere = pl.BlockSpec(memory_space=pltpu.HBM)
    turned = jnp.swapaxes(gradients, 2, 3)
    updates = pl.pallas_call(
        apply_kernel,
        grid=(BLOCKS // TOGETHER,),
        in_specs=[anywhere] * 8 + [pl.BlockSpec((2 * BLOCKS, W), lambda k: (0, 0)), block],
        out_specs=block,
        out_shape=jax.ShapeDtypeStruct(turned.shape, bf16),
        scratch_shapes=[
            pltpu.VMEM((BLOCKS, SIZE, HALF), bf16),
            pltpu.VMEM((TOGETHER, SIZE, SIZE), bf16),
            pltpu.SemaphoreType.DMA((BLOCKS // PART, 32)),
        ],
        compiler_params=pltpu.CompilerParams(dimension_semantics=("arbitrary",)),
        name="apply",
    )(*pieces, spine, turned)
    return jnp.swapaxes(updates, 2, 3)


def shift(value, axis, by):
    return lax.ppermute(value, axis, [(i, (i + by) % 4) for i in range(4)])


def swap_cores(value):
    return lax.ppermute(value, "c", [(0, 1), (1, 0)])


def crossed(value, stage, by):
    pairs = []
    for x in range(4):
        for z in range(4):
            for c in range(2):
                along_x = stage != c
                to = ((x + by) % 4, z) if along_x else (x, (z + by) % 4)
                pairs.append(((x * 4 + z) * 2 + c, (to[0] * 4 + to[1]) * 2 + c))
    return lax.ppermute(value, BLK, pairs)


def gather_pieces(piece):
    line = jnp.stack([piece] + [crossed(piece, 0, by) for by in SHIFTS[1:]])
    own = [line] + [crossed(line, 1, by) for by in SHIFTS[1:]]
    return own + [swap_cores(value) for value in own]


def per_device(statistics, gradients, live_counts, slot_row, sweeps):
    strips = roots(live_counts, sweeps, statistics)
    got = lax.all_to_all(strips, BLK, 0, 0, tiled=True)
    piece, spine, peak = select(live_counts, slot_row, got)
    peaks = [peak] + [shift(peak, "grp", by) for by in (1, 2, 3)]
    updates = apply(gather_pieces(piece), spine, gradients)
    off_max = jnp.max(jnp.stack([value[0, :MAXS] for value in peaks]), axis=0)
    return (updates, off_max)


def solution(mesh):
    split = Mesh(mesh.devices.reshape(4, 4, 2, mesh.shape["grp"]), BLK + ("grp",))
    return jax.shard_map(
        per_device,
        mesh=split,
        in_specs=(
            P("grp", BLK, None, None),
            P("grp", None, None, BLK),
            P("grp", None),
            P("grp", None),
            P("grp", BLK),
        ),
        out_specs=(P("grp", None, None, BLK), P()),
        check_vma=False,
    )
```

```python
import jax
import jax.numpy as jnp
from jax import lax
from jax.experimental import pallas as pl
from jax.experimental.pallas import tpu as pltpu
from jax.sharding import Mesh
from jax.sharding import PartitionSpec as P

MAXS = 2
SIZE = 512
W = 128
PAIRINGS = ((0, 1, 2, 3), (0, 2, 1, 3), (0, 3, 1, 2))
DAMPING = 0.01
SERIES_LIMIT = 1e-4
OFF_LEAST = 0.1
SPINE_LEAST = 0.1
bf16 = jnp.bfloat16
f32 = jnp.float32


def halves(x):
    high = x.astype(bf16)
    low = (x - high.astype(f32)).astype(bf16)
    return high, low


def dot1(left, right):
    return jnp.dot(left.astype(bf16), right.astype(bf16), preferred_element_type=f32)


def dot2(left, right):
    right = right.astype(bf16)
    return jnp.dot(
        jnp.concatenate(halves(left), axis=1),
        jnp.concatenate([right, right], axis=0),
        preferred_element_type=f32,
    )


def thirds(x):
    high, _ = halves(x)
    rest = x - high.astype(f32)
    middle, low = halves(rest)
    return high, middle, low


def dot6(left, right):
    a, b, c = thirds(left)
    x, y, z = thirds(right)
    return jnp.dot(
        jnp.concatenate([a, a, b, b, a, c], axis=1),
        jnp.concatenate([x, y, x, y, z, x], axis=0),
        preferred_element_type=f32,
    )


def angles_of(coupling, lower, upper):
    difference = upper - lower
    total = upper + lower
    bottom = difference * difference + 4.0 * coupling * coupling + DAMPING * (total * total)
    return coupling * difference / bottom


def span(member):
    return slice(member * W, member * W + W)


def eye(size):
    return lax.broadcasted_iota(jnp.int32, (size, size), 0) == lax.broadcasted_iota(
        jnp.int32, (size, size), 1
    )


def series_halves(items, checks):
    sides = [pair for a, at in items for pair in ((a, at), (at, a))]
    x1 = [0.25 * dot1(a, at) for a, at in sides]
    both = [dot1(x, jnp.concatenate([x, a], axis=1)) for x, (a, _) in zip(x1, sides)]
    x2 = [y[:, :W] for y in both]
    b1 = [a - y[:, W:] for y, (a, _) in zip(both, sides)]
    three = [dot1(y, jnp.concatenate([y, b, x], axis=1)) for y, b, x in zip(x2, b1, x1)]
    x4 = [y[:, :W] for y in three]
    b2 = [b + y[:, W : 2 * W] for b, y in zip(b1, three)]
    p0 = [y - x - z[:, 2 * W :] for x, y, z in zip(x1, x2, three)]
    last = [dot1(y, jnp.concatenate([b, p], axis=1)) for y, b, p in zip(x4, b2, p0)]
    ts = [b + y[:, :W] for b, y in zip(b2, last)]
    rs = [2.0 * (p + x + y[:, W:]) for p, x, y in zip(p0, x4, last)]
    for i, check in enumerate(checks):
        part = x4[2 * i] * x4[2 * i]
        check[...] += sum(part[8 * j : 8 * j + 8] for j in range(W // 8))
    return [(ts[2 * i], ts[2 * i + 1], rs[2 * i], rs[2 * i + 1]) for i in range(len(items))]


def newton_half(a, at):
    one = jnp.where(eye(W), 1.0, 0.0).astype(f32)
    s = one + 0.25 * dot6(a, at)
    norm = jnp.max(jnp.sum(jnp.abs(s), axis=1, keepdims=True), axis=0, keepdims=True)

    def step(_, y):
        return dot6(y, 2.0 * one - dot6(s, y))

    y = lax.fori_loop(0, 14, step, one * (2.0 / (1.0 + norm)))
    t = dot6(y, a)
    return t, t.T, -0.5 * dot6(t, at), -0.5 * dot6(at, t)


def one_round(states, pairing, exact):
    pairs = (pairing[:2], pairing[2:])
    diagonal = eye(W)
    mul, mul_v = (dot6, dot6) if exact else (dot1, dot2)
    keep = (lambda x: x) if exact else (lambda x: x.astype(bf16))
    items, checks = [], []
    for m, _, check in states:
        for p, q in pairs:
            dp = jnp.where(diagonal, m[span(p), span(p)], 0.0)
            dq = jnp.where(diagonal, m[span(q), span(q)], 0.0)
            row_p, row_q = (jnp.sum(d, axis=0, keepdims=True) for d in (dp, dq))
            col_p, col_q = (jnp.sum(d, axis=1, keepdims=True) for d in (dp, dq))
            a = angles_of(m[span(p), span(q)], col_p, row_q)
            at = angles_of(m[span(q), span(p)], row_p, col_q)
            items.append((a, at))
            checks.append(check)
    if exact:
        parts = [newton_half(*item) for item in items]
    else:
        parts = series_halves(items, checks)
    rs, rts = [], []
    for t, tt, r00, r11 in parts:
        rs.append(keep(jnp.concatenate(
            [jnp.concatenate([r00, t], axis=1), jnp.concatenate([-tt, r11], axis=1)], axis=0)))
        rts.append(keep(jnp.concatenate(
            [jnp.concatenate([r00, -t], axis=1), jnp.concatenate([tt, r11], axis=1)], axis=0)))

    def load(ref, rows, cols):
        return jnp.concatenate(
            [jnp.concatenate([ref[span(i), span(j)] for j in cols], axis=1) for i in rows], axis=0)

    def store(ref, rows, cols, value):
        for x, i in enumerate(rows):
            for y, j in enumerate(cols):
                ref[span(i), span(j)] = value[x * W : x * W + W, y * W : y * W + W]

    todo = [(i, x, y) for x, y in ((0, 1), (0, 0), (1, 1)) for i in range(len(states))]
    olds = [load(states[i][0], pairs[x], pairs[y]) for i, x, y in todo]
    gs = [old + mul(old, rs[2 * i + y]) for old, (i, x, y) in zip(olds, todo)]
    news = [g + mul(rts[2 * i + x], g) for g, (i, x, y) in zip(gs, todo)]
    for new, (i, x, y) in zip(news, todo):
        store(states[i][0], pairs[x], pairs[y], new)
        if x != y:
            store(states[i][0], pairs[y], pairs[x], new.T)
    for i, (_, v, _) in enumerate(states):
        for h, cols in enumerate(pairs):
            old = load(v, range(4), cols)
            store(v, range(4), cols, old + mul_v(old, rs[2 * i + h]))


def off_of(ref):
    square = ref[...] * ref[...]
    off = jnp.sum(jnp.where(eye(SIZE), 0.0, square), axis=0, keepdims=True)
    whole = jnp.sum(square, axis=0, keepdims=True)
    return jnp.sqrt(jnp.sum(off, axis=1, keepdims=True) / jnp.sum(whole, axis=1, keepdims=True))


def spine_of(value):
    size = value.shape[0]
    return jnp.sum(jnp.where(eye(size), value, 0.0), axis=0, keepdims=True)


HALF = SIZE // 2
STRIPS = 32
ROWS = SIZE // STRIPS
BLOCKS = 16
SHIFTS = (0, 1, 3, 2)
PART = 8
TOGETHER = 4
WIDE = 2 * HALF + W
BLK = ("x", "z", "c")


def roots_kernel(live_ref, sweeps_ref, stat_ref, out_ref, m, v, check, norms, before, extra):
    live = live_ref[0, lax.axis_index(BLK)]
    counts = [jnp.where(j < live, sweeps_ref[0, j], 0) for j in range(2)]
    lane = lax.broadcasted_iota(jnp.int32, (8, W), 1)
    norms[...] = jnp.zeros_like(norms)
    extra[...] = jnp.zeros_like(extra)

    def start(slot):
        m[slot] = stat_ref[0, slot]
        v[slot] = jnp.where(eye(SIZE), 1.0, 0.0).astype(f32)
        check[slot] = jnp.zeros((8, W), f32)
        norms[slot] = jnp.zeros((8, W), f32)
        before[slot] = jnp.broadcast_to(off_of(m.at[slot]), (8, W))

    def sweep_of(slots, exact):
        def sweep(s, carry):
            for pairing in PAIRINGS:
                one_round([(m.at[j], v.at[j], check.at[j]) for j in slots], pairing, exact)
            for j in slots:
                off = off_of(m.at[j])
                norms[j] = jnp.where(lane == s, off, norms[j])
                check[j] += jnp.where(off >= OFF_LEAST * before[j], 0.0, 1.0)
            return carry

        return sweep

    for j in range(2):

        @pl.when(counts[j] > 0)
        def _():
            start(j)

        @pl.when(counts[j] == 0)
        def _():
            cols = slice(j * HALF, j * HALF + HALF)
            out_ref[:, :, cols] = jnp.zeros((STRIPS, ROWS, HALF), bf16)

    common = jnp.minimum(counts[0], counts[1])
    longer = jnp.where(counts[0] >= counts[1], 0, 1)
    lax.fori_loop(0, common, sweep_of((0, 1), False), 0)
    lax.fori_loop(common, jnp.maximum(counts[0], counts[1]), sweep_of((longer,), False), 0)

    def again(slot, carry):
        count = jnp.where(slot == 0, counts[0], counts[1])

        @pl.when(count > 0)
        def _():
            least = SPINE_LEAST * spine_of(stat_ref[0, slot])
            shrunk = jnp.where(spine_of(m[slot]) >= least, 0.0, 1.0)
            fine = jnp.sum(check[slot]) + jnp.sum(shrunk) <= SERIES_LIMIT

            @pl.when(jnp.logical_not(fine))
            def _():
                start(slot)
                lax.fori_loop(0, count, sweep_of((slot,), True), 0)

        return carry

    lax.fori_loop(0, 2, again, 0)
    top, low = slice(0, HALF), slice(HALF, SIZE)
    for j in range(2):

        @pl.when(counts[j] > 0)
        def _():
            scale = lax.rsqrt(jnp.sqrt(spine_of(m[j])))

            def piece(rows, others):
                lh, ll = halves(v[j, rows] * scale)
                rh, rl = halves(v[j, others])
                return lax.dot_general(
                    jnp.concatenate([lh, ll, lh], axis=1),
                    jnp.concatenate([rh, rh, rl], axis=1),
                    (((1,), (1,)), ((), ())),
                    preferred_element_type=f32,
                )

            corner = piece(low, low)
            upper = lax.broadcasted_iota(jnp.int32, (HALF, HALF), 0) <= lax.broadcasted_iota(
                jnp.int32, (HALF, HALF), 1
            )
            folded = jnp.where(upper, piece(top, top), corner).astype(bf16)
            beyond = piece(top, low).astype(bf16)
            spine = spine_of(corner)
            cols = slice(j * HALF, j * HALF + HALF)
            out_ref[: STRIPS // 2, :, cols] = folded.reshape(STRIPS // 2, ROWS, HALF)
            out_ref[STRIPS // 2 :, :, cols] = beyond.reshape(STRIPS // 2, ROWS, HALF)
            extra[2 * j : 2 * j + 1] = spine[:, :W]
            extra[2 * j + 1 : 2 * j + 2] = spine[:, W:]

    for i, part in enumerate(thirds(jnp.maximum(norms[0, 0:1], norms[1, 0:1]))):
        extra[4 + i : 5 + i] = part.astype(f32)
    tile = extra[...].astype(bf16)
    for d in range(STRIPS):
        out_ref[d, :, 2 * HALF :] = tile


def roots(live_counts, sweeps, statistics):
    slots = statistics.shape[1]
    whole = pl.BlockSpec(memory_space=pltpu.VMEM)
    scalars = pl.BlockSpec(memory_space=pltpu.SMEM)
    return pl.pallas_call(
        roots_kernel,
        in_specs=[scalars, scalars, whole],
        out_specs=whole,
        scratch_shapes=[
            pltpu.VMEM((slots, SIZE, SIZE), f32),
            pltpu.VMEM((slots, SIZE, SIZE), f32),
            pltpu.VMEM((slots, 8, W), f32),
            pltpu.VMEM((slots, 8, W), f32),
            pltpu.VMEM((slots, 8, W), f32),
            pltpu.VMEM((ROWS, W), f32),
        ],
        out_shape=jax.ShapeDtypeStruct((STRIPS, ROWS, WIDE), bf16),
        name="roots",
    )(live_counts, sweeps, statistics)


def select_kernel(live_ref, row_ref, got_ref, *refs):
    piece_ref, spine_ref, peak_ref, table = refs

    def note(s, carry):
        @pl.when(s % 2 < live_ref[0, s // 2])
        def _():
            table[row_ref[0, s]] = s

        return carry

    lax.fori_loop(0, 2 * STRIPS, note, 0)
    peak = jnp.zeros((1, W), f32)
    for d in range(STRIPS):
        parts = got_ref[d, :, 2 * HALF :].astype(f32)
        peak = jnp.maximum(peak, parts[4:5] + parts[5:6] + parts[6:7])
    peak_ref[...] = jnp.broadcast_to(peak, (8, W))
    for k in range(BLOCKS):
        s = table[k]
        source = s // 2
        second = s % 2 == 1
        strip = jnp.where(second, got_ref[source, :, HALF : 2 * HALF], got_ref[source, :, :HALF])
        piece_ref[k] = strip
        parts = got_ref[source, :, 2 * HALF :].astype(f32)
        spine_ref[2 * k : 2 * k + 2] = jnp.where(second, parts[2:4], parts[0:2])


def select(live_counts, slot_row, got):
    whole = pl.BlockSpec(memory_space=pltpu.VMEM)
    scalars = pl.BlockSpec(memory_space=pltpu.SMEM)
    return pl.pallas_call(
        select_kernel,
        in_specs=[scalars, scalars, whole],
        out_specs=[whole] * 3,
        out_shape=[
            jax.ShapeDtypeStruct((BLOCKS, ROWS, HALF), bf16),
            jax.ShapeDtypeStruct((2 * BLOCKS, W), f32),
            jax.ShapeDtypeStruct((8, W), f32),
        ],
        scratch_shapes=[pltpu.SMEM((BLOCKS,), jnp.int32)],
        name="select",
    )(live_counts, slot_row, got)


def apply_kernel(*refs):
    pieces = refs[:8]
    spine_ref, grad_ref, out_ref, packed, full, sems = refs[8:]
    k = pl.program_id(0)
    x, z, c = (lax.axis_index(name) for name in BLK)

    def copies(part):
        for i, piece in enumerate(pieces):
            core, step = (c, 1 - c)[i // 4], i % 4
            for other in range(4):
                near, far = SHIFTS[other], SHIFTS[step]
                dx = far + core * (near - far)
                dz = near + core * (far - near)
                chip = ((x - dx + 4) % 4) * 4 + (z - dz + 4) % 4
                strip = chip * 2 + core
                yield pltpu.make_async_copy(
                    piece.at[other, pl.ds(part * PART, PART)],
                    packed.at[
                        pl.ds(part * PART, PART),
                        pl.ds(pl.multiple_of(strip * ROWS, ROWS), ROWS),
                    ],
                    sems.at[part, i * 4 + other],
                )

    @pl.when(k == 0)
    def _():
        for part in range(BLOCKS // PART):
            for copy in copies(part):
                copy.start()

    for part in range(BLOCKS // PART):

        @pl.when(k == part * PART // TOGETHER)
        def _():
            for copy in copies(part):
                copy.wait()

    one = jnp.where(eye(HALF), 1.0, 0.0).astype(bf16)
    across = lax.broadcasted_iota(jnp.int32, (HALF, HALF), 1)
    down = lax.broadcasted_iota(jnp.int32, (HALF, HALF), 0)

    def turned(x):
        return lax.dot_general(
            one, x, (((1,), (1,)), ((), ())), preferred_element_type=f32
        ).astype(bf16)

    for j in range(TOGETHER):
        block = k * TOGETHER + j
        folded, beyond = packed[block, :HALF], packed[block, HALF:]
        mirrored = turned(folded)
        pair = spine_ref[pl.ds(2 * block, 2)]
        spine = jnp.concatenate([pair[0:1], pair[1:2]], axis=1).astype(bf16)
        first = jnp.where(across >= down, folded, mirrored)
        last = jnp.where(across < down, folded, mirrored)
        last = jnp.where(across == down, jnp.broadcast_to(spine, (HALF, HALF)), last)
        full[j, :HALF, :HALF] = first
        full[j, :HALF, HALF:] = beyond
        full[j, HALF:, :HALF] = turned(beyond)
        full[j, HALF:, HALF:] = last
    for j in range(TOGETHER):
        value = jnp.dot(grad_ref[0, j], full[j], preferred_element_type=f32)
        out_ref[0, j] = value.astype(bf16)


def apply(pieces, spine, gradients):
    cols = gradients.shape[-1]
    block = pl.BlockSpec((1, TOGETHER, cols, SIZE), lambda k: (0, k, 0, 0))
    anywhere = pl.BlockSpec(memory_space=pltpu.HBM)
    turned = jnp.swapaxes(gradients, 2, 3)
    updates = pl.pallas_call(
        apply_kernel,
        grid=(BLOCKS // TOGETHER,),
        in_specs=[anywhere] * 8 + [pl.BlockSpec((2 * BLOCKS, W), lambda k: (0, 0)), block],
        out_specs=block,
        out_shape=jax.ShapeDtypeStruct(turned.shape, bf16),
        scratch_shapes=[
            pltpu.VMEM((BLOCKS, SIZE, HALF), bf16),
            pltpu.VMEM((TOGETHER, SIZE, SIZE), bf16),
            pltpu.SemaphoreType.DMA((BLOCKS // PART, 32)),
        ],
        compiler_params=pltpu.CompilerParams(dimension_semantics=("arbitrary",)),
        name="apply",
    )(*pieces, spine, turned)
    return jnp.swapaxes(updates, 2, 3)


def shift(value, axis, by):
    return lax.ppermute(value, axis, [(i, (i + by) % 4) for i in range(4)])


def swap_cores(value):
    return lax.ppermute(value, "c", [(0, 1), (1, 0)])


def crossed(value, stage, by):
    pairs = []
    for x in range(4):
        for z in range(4):
            for c in range(2):
                along_x = stage != c
                to = ((x + by) % 4, z) if along_x else (x, (z + by) % 4)
                pairs.append(((x * 4 + z) * 2 + c, (to[0] * 4 + to[1]) * 2 + c))
    return lax.ppermute(value, BLK, pairs)


def gather_pieces(piece, peak):
    line = jnp.stack([piece] + [crossed(piece, 0, by) for by in SHIFTS[1:]])
    own = [line] + [crossed(line, 1, by) for by in SHIFTS[1:]]
    peaks = [peak] + [shift(peak, "grp", by) for by in (1, 2, 3)]
    off_max = jnp.max(jnp.stack([value[0, :MAXS] for value in peaks]), axis=0)
    own[1], off_max = lax.optimization_barrier((own[1], off_max))
    return own + [swap_cores(value) for value in own], off_max


def per_device(statistics, gradients, live_counts, slot_row, sweeps):
    strips = roots(live_counts, sweeps, statistics)
    got = lax.all_to_all(strips, BLK, 0, 0, tiled=True)
    piece, spine, peak = select(live_counts, slot_row, got)
    pieces, off_max = gather_pieces(piece, peak)
    updates = apply(pieces, spine, gradients)
    return (updates, off_max)


def solution(mesh):
    split = Mesh(mesh.devices.reshape(4, 4, 2, mesh.shape["grp"]), BLK + ("grp",))
    return jax.shard_map(
        per_device,
        mesh=split,
        in_specs=(
            P("grp", BLK, None, None),
            P("grp", None, None, BLK),
            P("grp", None),
            P("grp", None),
            P("grp", BLK),
        ),
        out_specs=(P("grp", None, None, BLK), P()),
        check_vma=False,
    )
```

```python
import jax
import jax.numpy as jnp
from jax import lax
from jax.experimental import pallas as pl
from jax.experimental.pallas import tpu as pltpu
from jax.sharding import Mesh
from jax.sharding import PartitionSpec as P

MAXS = 2
SIZE = 512
W = 128
PAIRINGS = ((0, 1, 2, 3), (0, 2, 1, 3), (0, 3, 1, 2))
DAMPING = 0.01
SERIES_LIMIT = 1e-4
OFF_LEAST = 0.1
SPINE_LEAST = 0.1
bf16 = jnp.bfloat16
f32 = jnp.float32


def halves(x):
    high = x.astype(bf16)
    low = (x - high.astype(f32)).astype(bf16)
    return high, low


def dot1(left, right):
    return jnp.dot(left.astype(bf16), right.astype(bf16), preferred_element_type=f32)


def dot2(left, right):
    right = right.astype(bf16)
    return jnp.dot(
        jnp.concatenate(halves(left), axis=1),
        jnp.concatenate([right, right], axis=0),
        preferred_element_type=f32,
    )


def thirds(x):
    high, _ = halves(x)
    rest = x - high.astype(f32)
    middle, low = halves(rest)
    return high, middle, low


def dot6(left, right):
    a, b, c = thirds(left)
    x, y, z = thirds(right)
    return jnp.dot(
        jnp.concatenate([a, a, b, b, a, c], axis=1),
        jnp.concatenate([x, y, x, y, z, x], axis=0),
        preferred_element_type=f32,
    )


def angles_of(coupling, lower, upper):
    difference = upper - lower
    total = upper + lower
    bottom = difference * difference + 4.0 * coupling * coupling + DAMPING * (total * total)
    return coupling * difference / bottom


def span(member):
    return slice(member * W, member * W + W)


def eye(size):
    return lax.broadcasted_iota(jnp.int32, (size, size), 0) == lax.broadcasted_iota(
        jnp.int32, (size, size), 1
    )


def series_halves(items, checks):
    sides = [pair for a, at in items for pair in ((a, at), (at, a))]
    x1 = [0.25 * dot1(a, at) for a, at in sides]
    both = [dot1(x, jnp.concatenate([x, a], axis=1)) for x, (a, _) in zip(x1, sides)]
    x2 = [y[:, :W] for y in both]
    b1 = [a - y[:, W:] for y, (a, _) in zip(both, sides)]
    three = [dot1(y, jnp.concatenate([y, b, x], axis=1)) for y, b, x in zip(x2, b1, x1)]
    x4 = [y[:, :W] for y in three]
    b2 = [b + y[:, W : 2 * W] for b, y in zip(b1, three)]
    p0 = [y - x - z[:, 2 * W :] for x, y, z in zip(x1, x2, three)]
    last = [dot1(y, jnp.concatenate([b, p], axis=1)) for y, b, p in zip(x4, b2, p0)]
    ts = [b + y[:, :W] for b, y in zip(b2, last)]
    rs = [2.0 * (p + x + y[:, W:]) for p, x, y in zip(p0, x4, last)]
    for i, check in enumerate(checks):
        part = x4[2 * i] * x4[2 * i]
        check[...] += sum(part[8 * j : 8 * j + 8] for j in range(W // 8))
    return [(ts[2 * i], ts[2 * i + 1], rs[2 * i], rs[2 * i + 1]) for i in range(len(items))]


def newton_half(a, at):
    one = jnp.where(eye(W), 1.0, 0.0).astype(f32)
    s = one + 0.25 * dot6(a, at)
    norm = jnp.max(jnp.sum(jnp.abs(s), axis=1, keepdims=True), axis=0, keepdims=True)

    def step(_, y):
        return dot6(y, 2.0 * one - dot6(s, y))

    y = lax.fori_loop(0, 14, step, one * (2.0 / (1.0 + norm)))
    t = dot6(y, a)
    return t, t.T, -0.5 * dot6(t, at), -0.5 * dot6(at, t)


def one_round(states, pairing, exact):
    pairs = (pairing[:2], pairing[2:])
    diagonal = eye(W)
    mul, mul_v = (dot6, dot6) if exact else (dot1, dot2)
    keep = (lambda x: x) if exact else (lambda x: x.astype(bf16))
    items, checks = [], []
    for m, _, check in states:
        for p, q in pairs:
            dp = jnp.where(diagonal, m[span(p), span(p)], 0.0)
            dq = jnp.where(diagonal, m[span(q), span(q)], 0.0)
            row_p, row_q = (jnp.sum(d, axis=0, keepdims=True) for d in (dp, dq))
            col_p, col_q = (jnp.sum(d, axis=1, keepdims=True) for d in (dp, dq))
            a = angles_of(m[span(p), span(q)], col_p, row_q)
            at = angles_of(m[span(q), span(p)], row_p, col_q)
            items.append((a, at))
            checks.append(check)
    if exact:
        parts = [newton_half(*item) for item in items]
    else:
        parts = series_halves(items, checks)
    rs, rts = [], []
    for t, tt, r00, r11 in parts:
        rs.append(keep(jnp.concatenate(
            [jnp.concatenate([r00, t], axis=1), jnp.concatenate([-tt, r11], axis=1)], axis=0)))
        rts.append(keep(jnp.concatenate(
            [jnp.concatenate([r00, -t], axis=1), jnp.concatenate([tt, r11], axis=1)], axis=0)))

    def load(ref, rows, cols):
        return jnp.concatenate(
            [jnp.concatenate([ref[span(i), span(j)] for j in cols], axis=1) for i in rows], axis=0)

    def store(ref, rows, cols, value):
        for x, i in enumerate(rows):
            for y, j in enumerate(cols):
                ref[span(i), span(j)] = value[x * W : x * W + W, y * W : y * W + W]

    todo = [(i, x, y) for x, y in ((0, 1), (0, 0), (1, 1)) for i in range(len(states))]
    olds = [load(states[i][0], pairs[x], pairs[y]) for i, x, y in todo]
    gs = [old + mul(old, rs[2 * i + y]) for old, (i, x, y) in zip(olds, todo)]
    news = [g + mul(rts[2 * i + x], g) for g, (i, x, y) in zip(gs, todo)]
    for new, (i, x, y) in zip(news, todo):
        store(states[i][0], pairs[x], pairs[y], new)
        if x != y:
            store(states[i][0], pairs[y], pairs[x], new.T)
    for i, (_, v, _) in enumerate(states):
        for h, cols in enumerate(pairs):
            old = load(v, range(4), cols)
            store(v, range(4), cols, old + mul_v(old, rs[2 * i + h]))


def off_of(ref):
    square = ref[...] * ref[...]
    off = jnp.sum(jnp.where(eye(SIZE), 0.0, square), axis=0, keepdims=True)
    whole = jnp.sum(square, axis=0, keepdims=True)
    return jnp.sqrt(jnp.sum(off, axis=1, keepdims=True) / jnp.sum(whole, axis=1, keepdims=True))


def spine_of(value):
    size = value.shape[0]
    return jnp.sum(jnp.where(eye(size), value, 0.0), axis=0, keepdims=True)


HALF = SIZE // 2
STRIPS = 32
ROWS = SIZE // STRIPS
BLOCKS = 16
SHIFTS = (0, 1, 3, 2)
PART = 8
TOGETHER = 4
WIDE = 2 * HALF + W
BLK = ("x", "z", "c")


def roots_kernel(live_ref, sweeps_ref, stat_ref, out_ref, m, v, check, norms, before, extra):
    live = live_ref[0, lax.axis_index(BLK)]
    counts = [jnp.where(j < live, sweeps_ref[0, j], 0) for j in range(2)]
    lane = lax.broadcasted_iota(jnp.int32, (8, W), 1)
    norms[...] = jnp.zeros_like(norms)
    extra[...] = jnp.zeros_like(extra)

    def start(slot):
        m[slot] = stat_ref[0, slot]
        v[slot] = jnp.where(eye(SIZE), 1.0, 0.0).astype(f32)
        check[slot] = jnp.zeros((8, W), f32)
        norms[slot] = jnp.zeros((8, W), f32)
        before[slot] = jnp.broadcast_to(off_of(m.at[slot]), (8, W))

    def sweep_of(slots, exact):
        def sweep(s, carry):
            for pairing in PAIRINGS:
                one_round([(m.at[j], v.at[j], check.at[j]) for j in slots], pairing, exact)
            for j in slots:
                off = off_of(m.at[j])
                norms[j] = jnp.where(lane == s, off, norms[j])
                check[j] += jnp.where(off >= OFF_LEAST * before[j], 0.0, 1.0)
            return carry

        return sweep

    for j in range(2):

        @pl.when(counts[j] > 0)
        def _():
            start(j)

        @pl.when(counts[j] == 0)
        def _():
            cols = slice(j * HALF, j * HALF + HALF)
            out_ref[:, :, cols] = jnp.zeros((STRIPS, ROWS, HALF), bf16)

    common = jnp.minimum(counts[0], counts[1])
    longer = jnp.where(counts[0] >= counts[1], 0, 1)
    lax.fori_loop(0, common, sweep_of((0, 1), False), 0)
    lax.fori_loop(common, jnp.maximum(counts[0], counts[1]), sweep_of((longer,), False), 0)

    def again(slot, carry):
        count = jnp.where(slot == 0, counts[0], counts[1])

        @pl.when(count > 0)
        def _():
            least = SPINE_LEAST * spine_of(stat_ref[0, slot])
            shrunk = jnp.where(spine_of(m[slot]) >= least, 0.0, 1.0)
            fine = jnp.sum(check[slot]) + jnp.sum(shrunk) <= SERIES_LIMIT

            @pl.when(jnp.logical_not(fine))
            def _():
                start(slot)
                lax.fori_loop(0, count, sweep_of((slot,), True), 0)

        return carry

    lax.fori_loop(0, 2, again, 0)
    top, low = slice(0, HALF), slice(HALF, SIZE)
    for j in range(2):

        @pl.when(counts[j] > 0)
        def _():
            scale = lax.rsqrt(jnp.sqrt(spine_of(m[j])))

            def piece(rows, others):
                lh, ll = halves(v[j, rows] * scale)
                rh, rl = halves(v[j, others])
                return lax.dot_general(
                    jnp.concatenate([lh, ll, lh], axis=1),
                    jnp.concatenate([rh, rh, rl], axis=1),
                    (((1,), (1,)), ((), ())),
                    preferred_element_type=f32,
                )

            corner = piece(low, low)
            upper = lax.broadcasted_iota(jnp.int32, (HALF, HALF), 0) <= lax.broadcasted_iota(
                jnp.int32, (HALF, HALF), 1
            )
            folded = jnp.where(upper, piece(top, top), corner).astype(bf16)
            beyond = piece(top, low).astype(bf16)
            spine = spine_of(corner)
            cols = slice(j * HALF, j * HALF + HALF)
            out_ref[: STRIPS // 2, :, cols] = folded.reshape(STRIPS // 2, ROWS, HALF)
            out_ref[STRIPS // 2 :, :, cols] = beyond.reshape(STRIPS // 2, ROWS, HALF)
            extra[2 * j : 2 * j + 1] = spine[:, :W]
            extra[2 * j + 1 : 2 * j + 2] = spine[:, W:]

    for i, part in enumerate(thirds(jnp.maximum(norms[0, 0:1], norms[1, 0:1]))):
        extra[4 + i : 5 + i] = part.astype(f32)
    tile = extra[...].astype(bf16)
    for d in range(STRIPS):
        out_ref[d, :, 2 * HALF :] = tile


def roots(live_counts, sweeps, statistics):
    slots = statistics.shape[1]
    whole = pl.BlockSpec(memory_space=pltpu.VMEM)
    scalars = pl.BlockSpec(memory_space=pltpu.SMEM)
    return pl.pallas_call(
        roots_kernel,
        in_specs=[scalars, scalars, whole],
        out_specs=whole,
        scratch_shapes=[
            pltpu.VMEM((slots, SIZE, SIZE), f32),
            pltpu.VMEM((slots, SIZE, SIZE), f32),
            pltpu.VMEM((slots, 8, W), f32),
            pltpu.VMEM((slots, 8, W), f32),
            pltpu.VMEM((slots, 8, W), f32),
            pltpu.VMEM((ROWS, W), f32),
        ],
        out_shape=jax.ShapeDtypeStruct((STRIPS, ROWS, WIDE), bf16),
        name="roots",
    )(live_counts, sweeps, statistics)


def select_kernel(live_ref, row_ref, got_ref, *refs):
    piece_ref, spine_ref, peak_ref, table = refs

    def note(s, carry):
        @pl.when(s % 2 < live_ref[0, s // 2])
        def _():
            table[row_ref[0, s]] = s

        return carry

    lax.fori_loop(0, 2 * STRIPS, note, 0)
    peak = jnp.zeros((1, W), f32)
    for d in range(STRIPS):
        parts = got_ref[d, :, 2 * HALF :].astype(f32)
        peak = jnp.maximum(peak, parts[4:5] + parts[5:6] + parts[6:7])
    peak_ref[...] = jnp.broadcast_to(peak, (8, W))
    for k in range(BLOCKS):
        s = table[k]
        source = s // 2
        second = s % 2 == 1
        strip = jnp.where(second, got_ref[source, :, HALF : 2 * HALF], got_ref[source, :, :HALF])
        piece_ref[k] = strip
        parts = got_ref[source, :, 2 * HALF :].astype(f32)
        spine_ref[2 * k : 2 * k + 2] = jnp.where(second, parts[2:4], parts[0:2])


def select(live_counts, slot_row, got):
    whole = pl.BlockSpec(memory_space=pltpu.VMEM)
    scalars = pl.BlockSpec(memory_space=pltpu.SMEM)
    return pl.pallas_call(
        select_kernel,
        in_specs=[scalars, scalars, whole],
        out_specs=[whole] * 3,
        out_shape=[
            jax.ShapeDtypeStruct((BLOCKS, ROWS, HALF), bf16),
            jax.ShapeDtypeStruct((2 * BLOCKS, W), f32),
            jax.ShapeDtypeStruct((8, W), f32),
        ],
        scratch_shapes=[pltpu.SMEM((BLOCKS,), jnp.int32)],
        name="select",
    )(live_counts, slot_row, got)


def apply_kernel(*refs):
    pieces = refs[:8]
    spine_ref, grad_ref, out_ref, packed, full, sems = refs[8:]
    k = pl.program_id(0)
    x, z, c = (lax.axis_index(name) for name in BLK)

    def copies(part):
        for i, piece in enumerate(pieces):
            core, step = (c, 1 - c)[i // 4], i % 4
            for other in range(4):
                near, far = SHIFTS[other], SHIFTS[step]
                dx = far + core * (near - far)
                dz = near + core * (far - near)
                chip = ((x - dx + 4) % 4) * 4 + (z - dz + 4) % 4
                strip = chip * 2 + core
                yield pltpu.make_async_copy(
                    piece.at[other, pl.ds(part * PART, PART)],
                    packed.at[
                        pl.ds(part * PART, PART),
                        pl.ds(pl.multiple_of(strip * ROWS, ROWS), ROWS),
                    ],
                    sems.at[part, i * 4 + other],
                )

    @pl.when(k == 0)
    def _():
        for part in range(BLOCKS // PART):
            for copy in copies(part):
                copy.start()

    for part in range(BLOCKS // PART):

        @pl.when(k == part * PART // TOGETHER)
        def _():
            for copy in copies(part):
                copy.wait()

    one = jnp.where(eye(HALF), 1.0, 0.0).astype(bf16)
    across = lax.broadcasted_iota(jnp.int32, (HALF, HALF), 1)
    down = lax.broadcasted_iota(jnp.int32, (HALF, HALF), 0)

    def turned(x):
        return lax.dot_general(
            one, x, (((1,), (1,)), ((), ())), preferred_element_type=f32
        ).astype(bf16)

    for j in range(TOGETHER):
        block = k * TOGETHER + j
        folded, beyond = packed[block, :HALF], packed[block, HALF:]
        mirrored = turned(folded)
        pair = spine_ref[pl.ds(2 * block, 2)]
        spine = jnp.concatenate([pair[0:1], pair[1:2]], axis=1).astype(bf16)
        first = jnp.where(across >= down, folded, mirrored)
        last = jnp.where(across < down, folded, mirrored)
        last = jnp.where(across == down, jnp.broadcast_to(spine, (HALF, HALF)), last)
        full[j, :HALF, :HALF] = first
        full[j, :HALF, HALF:] = beyond
        full[j, HALF:, :HALF] = turned(beyond)
        full[j, HALF:, HALF:] = last
    for j in range(TOGETHER):
        value = jnp.dot(grad_ref[0, j], full[j], preferred_element_type=f32)
        out_ref[0, j] = value.astype(bf16)


def apply(pieces, spine, gradients):
    cols = gradients.shape[-1]
    block = pl.BlockSpec((1, TOGETHER, cols, SIZE), lambda k: (0, k, 0, 0))
    anywhere = pl.BlockSpec(memory_space=pltpu.HBM)
    turned = jnp.swapaxes(gradients, 2, 3)
    updates = pl.pallas_call(
        apply_kernel,
        grid=(BLOCKS // TOGETHER,),
        in_specs=[anywhere] * 8 + [pl.BlockSpec((2 * BLOCKS, W), lambda k: (0, 0)), block],
        out_specs=block,
        out_shape=jax.ShapeDtypeStruct(turned.shape, bf16),
        scratch_shapes=[
            pltpu.VMEM((BLOCKS, SIZE, HALF), bf16),
            pltpu.VMEM((TOGETHER, SIZE, SIZE), bf16),
            pltpu.SemaphoreType.DMA((BLOCKS // PART, 32)),
        ],
        compiler_params=pltpu.CompilerParams(dimension_semantics=("arbitrary",)),
        name="apply",
    )(*pieces, spine, turned)
    return jnp.swapaxes(updates, 2, 3)


def shift(value, axis, by):
    return lax.ppermute(value, axis, [(i, (i + by) % 4) for i in range(4)])


def swap_cores(value):
    return lax.ppermute(value, "c", [(0, 1), (1, 0)])


def crossed(value, stage, by):
    pairs = []
    for x in range(4):
        for z in range(4):
            for c in range(2):
                along_x = stage != c
                to = ((x + by) % 4, z) if along_x else (x, (z + by) % 4)
                pairs.append(((x * 4 + z) * 2 + c, (to[0] * 4 + to[1]) * 2 + c))
    return lax.ppermute(value, BLK, pairs)


def gather_pieces(piece, peak):
    line = jnp.stack([piece] + [crossed(piece, 0, by) for by in SHIFTS[1:]])
    own = [line] + [crossed(line, 1, by) for by in SHIFTS[1:]]
    peaks = [peak] + [shift(peak, "grp", by) for by in (1, 2, 3)]
    off_max = jnp.max(jnp.stack([value[0, :MAXS] for value in peaks]), axis=0)
    own[3], off_max = lax.optimization_barrier((own[3], off_max))
    return own + [swap_cores(value) for value in own], off_max


def per_device(statistics, gradients, live_counts, slot_row, sweeps):
    strips = roots(live_counts, sweeps, statistics)
    got = lax.all_to_all(strips, BLK, 0, 0, tiled=True)
    piece, spine, peak = select(live_counts, slot_row, got)
    pieces, off_max = gather_pieces(piece, peak)
    updates = apply(pieces, spine, gradients)
    return (updates, off_max)


def solution(mesh):
    split = Mesh(mesh.devices.reshape(4, 4, 2, mesh.shape["grp"]), BLK + ("grp",))
    return jax.shard_map(
        per_device,
        mesh=split,
        in_specs=(
            P("grp", BLK, None, None),
            P("grp", None, None, BLK),
            P("grp", None),
            P("grp", None),
            P("grp", BLK),
        ),
        out_specs=(P("grp", None, None, BLK), P()),
        check_vma=False,
    )
```
